32 devices in a mesh: section: 8 (over y, x, core), tensor: 4 (over z).
Axes of the slice: x: 2, y: 2, z: 4, core: 2. Of those that a mesh axis runs over, the one named last changes fastest.
Arguments:
- matching: int32 [8], replicated, may hold values from 0 to 7, each once
- lengths: int32 [32], replicated, may hold values from 2 to 255
- queries: bfloat16 [8, 32, 8192], P('section', None, 'tensor'), may hold values from -200 to 200
- kv_cache: bfloat16 [8, 32, 256, 2048], P('section', None, None, 'tensor'), may hold values from -6 to 6
- incoming_key_value: bfloat16 [8, 32, 2048], P('section', None, 'tensor'), may hold values from -6 to 6
- residual: bfloat16 [8, 32, 8192], P('section', None, 'tensor'), may hold values from -6 to 6
- out_weight: bfloat16 [8, 8192, 8192], P('section', 'tensor'), may hold values from -0.09375 to 0.09375
- norm_gain: bfloat16 [8, 8192], P('section', 'tensor'), may hold values from 0.5 to 1.5
Outputs:
- cache_out: bfloat16 [8, 32, 256, 2048], P('section', None, None, 'tensor')
- stream_out: bfloat16 [8, 32, 8192], P('section', None, 'tensor')
- normed_out: bfloat16 [8, 32, 8192], P('section', None, 'tensor')
The draws below stay inside these ranges and needn't reach their ends.
All inputs are finite; a program needn't handle non-finite values.
Results may differ from the reference program's by a relative error of at most 0.0042.
Values may be sent and summed in bfloat16 or wider, within the bound.
No kernel may reach another device: no remote copies, remote signals or barrier semaphores. Data moves between devices by JAX's collectives and lax.ppermute only.
A program may use at most 128 MiB of HBM per device.

```python
import math
import jax
import jax.numpy as jnp
from jax import lax

D = 8192
QUERY_HEADS = 64
KEY_VALUE_HEADS = 8
HEAD_SIZE = 128
BATCH_SEQUENCES = 32
CONTEXT_SLOTS = 256
LAYER_COUNT = 8
QUERY_PER_KEY = 8
N_SECTION = 8


def leading_keys(key):
    return jnp.clip(jax.random.normal(jax.random.fold_in(key, 11), (LAYER_COUNT, BATCH_SEQUENCES, 2, KEY_VALUE_HEADS * 2 * HEAD_SIZE), jnp.float32), -6.0, 6.0)


def draw_kv_cache(key, part):
    slots_per_head = leading_keys(key)
    remaining_slots = jnp.clip(jax.random.normal(jax.random.fold_in(key, 12), (LAYER_COUNT, BATCH_SEQUENCES, CONTEXT_SLOTS - 2, KEY_VALUE_HEADS * 2 * HEAD_SIZE), jnp.float32), -6.0, 6.0)
    return jnp.concatenate([slots_per_head, remaining_slots], axis=2).astype(jnp.bfloat16)


def draw_queries(key, part):
    base = jnp.clip(jax.random.normal(jax.random.fold_in(key, 13), (LAYER_COUNT, BATCH_SEQUENCES, QUERY_HEADS * HEAD_SIZE), jnp.float32), -6.0, 6.0)
    return base.astype(jnp.bfloat16)


def set_ends(result, rng, low, largest):
    extent = result.shape
    spot = [jax.random.randint(jax.random.fold_in(rng, axis), (), 0, extent[axis]) for axis in range(len(extent))]
    result = result.at[tuple(spot)].set(low)
    longest = extent.index(max(extent))
    spot[longest] = (spot[longest] + 1) % extent[longest]
    return result.at[tuple(spot)].set(largest)


def raised(result, stream_key, source, target, parts, factor):
    owner, partner = [(jnp.arange(result.shape[axis_at]) // (result.shape[axis_at] // parts)).reshape([-1 if axis == axis_at else 1 for axis in range(result.ndim)]) for axis_at in (source, target)]
    chosen = jax.random.permutation(stream_key, parts)[partner]
    strong = (owner == chosen) | (owner == (partner + parts // 2) % parts)
    return jnp.where(strong, factor * result, result)


def shard_levels(key, dims, pieces, smallest, high):
    factor_of = 1.0
    for axis_at, shards_of in pieces:
        draws = jax.random.uniform(jax.random.fold_in(jax.random.fold_in(key, 6), axis_at), (shards_of,), jnp.float32, smallest / len(pieces), high / len(pieces))
        factor_of = factor_of * jnp.repeat(jnp.exp(draws), dims[axis_at] // shards_of).reshape((-1,) + (1,) * (len(dims) - 1 - axis_at))
    return factor_of


def noise(rng, extent, width, most, pieces=(), held_as=jnp.bfloat16):
    entries = width * jax.random.normal(rng, extent, jnp.float32)
    if pieces:
        entries = entries * shard_levels(rng, extent, pieces, -0.22, 0.18)
    return jnp.clip(entries, -most, most).astype(held_as)


def noise_with(key, extent, scale, most, split, heavy, kind=jnp.bfloat16):
    values = scale * jax.random.normal(key, extent, jnp.float32)
    if split:
        values = values * shard_levels(key, extent, split, -0.22, 0.18)
    return jnp.clip(raised(values, jax.random.fold_in(key, 3), *heavy), -most, most).astype(kind)


def setup_inputs(seed: int = 0) -> dict:
    splits = jax.random.split(jax.random.key(seed), 9)
    matching = jax.random.permutation(splits[0], N_SECTION).astype(jnp.int32)
    lengths = set_ends(jax.random.randint(splits[1], (BATCH_SEQUENCES,), 2, CONTEXT_SLOTS), jax.random.fold_in(splits[1], 1), 2, CONTEXT_SLOTS - 1).astype(jnp.int32)
    queries = draw_queries(jax.random.fold_in(splits[8], 71), 0)
    kv_cache = draw_kv_cache(jax.random.fold_in(splits[8], 71), 0)
    incoming_key_value = noise(splits[4], (LAYER_COUNT, BATCH_SEQUENCES, KEY_VALUE_HEADS * 2 * HEAD_SIZE), 1.0, 6.0, ((0, 8), (2, 4)))
    residual = noise(splits[5], (LAYER_COUNT, BATCH_SEQUENCES, D), 1.0, 6.0, ((0, 8), (2, 4)))
    out_weight = noise_with(splits[6], (LAYER_COUNT, QUERY_HEADS * HEAD_SIZE, D), (QUERY_HEADS * HEAD_SIZE) ** -0.5, 0.09375, ((0, 8), (1, 4)), (1, 2, 4, 2.0))
    norm_gain = jnp.clip(1.0 + 0.1 * jax.random.normal(splits[7], (LAYER_COUNT, D), jnp.float32), 0.5, 1.5).astype(jnp.bfloat16)
    return {"matching": matching, "lengths": lengths, "queries": queries, "kv_cache": kv_cache, "incoming_key_value": incoming_key_value, "residual": residual, "out_weight": out_weight, "norm_gain": norm_gain}


def layer_step(query_vectors, cache_rows, fresh_rows, residual_rows, projection, gain_row, lengths):
    places = jnp.arange(CONTEXT_SLOTS, dtype=jnp.int32)
    written = places[None, :] == lengths[:, None]
    updated_cache = jnp.where(written[:, :, None], fresh_rows[:, None, :], cache_rows)
    heads_separated = updated_cache.reshape(BATCH_SEQUENCES, CONTEXT_SLOTS, KEY_VALUE_HEADS, 2, HEAD_SIZE)
    key_rows = heads_separated[:, :, :, 0].astype(jnp.float32)
    value_rows = heads_separated[:, :, :, 1].astype(jnp.float32)
    grouped_queries = query_vectors.reshape(BATCH_SEQUENCES, KEY_VALUE_HEADS, QUERY_PER_KEY, HEAD_SIZE).astype(jnp.float32)
    scores = jnp.einsum('bgrd,bsgd->bgrs', grouped_queries, key_rows) / math.sqrt(HEAD_SIZE)
    visible = places[None, :] <= lengths[:, None]
    scores = jnp.where(visible[:, None, None, :], scores, -1e+30)
    weights = jax.nn.softmax(scores, axis=-1).astype(jnp.bfloat16)
    attended = jnp.einsum('bgrs,bsgd->bgrd', weights.astype(jnp.float32), value_rows).astype(jnp.bfloat16)
    partial_value = jnp.dot(attended.reshape(BATCH_SEQUENCES, QUERY_HEADS * HEAD_SIZE), projection, preferred_element_type=jnp.float32)
    stream = residual_rows.astype(jnp.float32) + partial_value
    scale = lax.rsqrt(lax.optimization_barrier(jnp.mean(stream * stream, axis=-1, keepdims=True)) + 1e-05)
    normed = stream * scale * gain_row.astype(jnp.float32)
    return (updated_cache, stream.astype(jnp.bfloat16), normed.astype(jnp.bfloat16))

def reference(matching, lengths, queries, kv_cache, incoming_key_value, residual, out_weight, norm_gain):

    def one_layer(layer_idx):
        return layer_step(queries[layer_idx], kv_cache[layer_idx], incoming_key_value[layer_idx], residual[layer_idx], out_weight[layer_idx], norm_gain[layer_idx], lengths)
    cache_out, stream_out, normed_out = lax.map(one_layer, matching)
    return (cache_out, stream_out, normed_out)
```

```python
import functools
import itertools
import math
import random

import jax
import jax.numpy as jnp
import numpy as np
from jax import lax
from jax.experimental import pallas as pl
from jax.experimental.pallas import tpu as pltpu
from jax.sharding import PartitionSpec as P


D = 8192
HEAD_SIZE = 128
PIECES = 4
STREAMS = 2
MAX_ROUNDS = 8
BASE_ROUNDS = 4
FIELDS = 2 * MAX_ROUNDS + 8 * PIECES
RING = (0, 1, 3, 2)


def ring_path(source, target, clockwise):
    at = RING.index(source)
    hops = []
    while RING[at] != target:
        later = (at + (1 if clockwise else -1)) % 4
        hops.append((RING[at], RING[later]))
        at = later
    return hops


def demand_classes():
    pairs = [(a, b) for a in range(4) for b in range(a, 4)]
    return [
        combo
        for combo in itertools.product(pairs, repeat=4)
        if all(sum(pair.count(chip) for pair in combo) == 2 for chip in range(4))
    ]


def split_directions(items, rng):
    share = {}
    for source, which, target in items:
        gap = (RING.index(target) - RING.index(source)) % 4
        share[(source, which)] = {1: PIECES, 2: PIECES // 2, 3: 0}[gap]

    def cost():
        load = {}
        for source, which, target in items:
            count = share[(source, which)]
            for hop in ring_path(source, target, True):
                load[hop] = load.get(hop, 0) + count
            for hop in ring_path(source, target, False):
                load[hop] = load.get(hop, 0) + PIECES - count
        return (max(load.values(), default=0), sum(v * v for v in load.values()))

    keys = list(share)
    single = [((key, step),) for key in keys for step in (1, -1, 2, -2)]
    double = [
        ((key, a), (other, b))
        for key, other in itertools.combinations(keys, 2)
        for a in (1, -1)
        for b in (1, -1)
    ]
    best = cost()
    improved = True
    while improved:
        improved = False
        moves = single + double
        rng.shuffle(moves)
        for move in moves:
            if any(not 0 <= share[key] + step <= PIECES for key, step in move):
                continue
            for key, step in move:
                share[key] += step
            now = cost()
            if now < best:
                best = now
                improved = True
                break
            for key, step in move:
                share[key] -= step
    return (share, best[0])


def schedule_rounds(items, share, rng, noise):
    pieces = []
    for source, which, target in items:
        for number in range(PIECES):
            hops = ring_path(source, target, number < share[(source, which)])
            pieces.append([hops, 0, 0, (source, which, number)])
    rounds = []
    while any(piece[1] < len(piece[0]) for piece in pieces):
        taken = {}
        for piece in sorted(
            pieces, key=lambda piece: piece[1] - len(piece[0]) + noise * rng.random()
        ):
            if piece[1] < len(piece[0]) and piece[2] <= len(rounds):
                taken.setdefault(piece[0][piece[1]], piece)
        for piece in taken.values():
            piece[1] += 1
            piece[2] = len(rounds) + 1
        rounds.append({hop: piece[3] for hop, piece in taken.items()})
    return rounds


def solve_class(combo, tries=60):
    rng = random.Random(7)
    items = [
        (source, which, target)
        for source, pair in enumerate(combo)
        for which, target in enumerate(pair)
        if source != target
    ]
    best = None
    for attempt in range(tries):
        if attempt % 5 == 0:
            share, bound = split_directions(items, rng)
        rounds = schedule_rounds(items, share, rng, (0.5, 1.0, 1.0, 1.5, 2.5)[attempt % 5])
        if best is None or len(rounds) < len(best):
            best = rounds
        if len(best) <= bound:
            break
    assert len(best) <= MAX_ROUNDS
    return best


@functools.cache
def routing_tables():
    classes = demand_classes()
    index = np.zeros((1000,), np.int32)
    rows = np.zeros((len(classes), 2, 128), np.int32)
    for number, combo in enumerate(classes):
        ids = [lo * (7 - lo) // 2 + hi for lo, hi in combo]
        index[ids[0] + 10 * ids[1] + 100 * ids[2]] = number
        where = {
            (chip, which, piece): (chip, which * PIECES + piece)
            for chip in range(4)
            for which in range(2)
            for piece in range(PIECES)
        }
        flat = np.zeros((256,), np.int32)
        rounds = solve_class(combo)
        for step, taken in enumerate(rounds):
            for (source, target), piece in taken.items():
                across = 0 if source ^ target == 1 else 1
                chip, slot = where[piece]
                assert chip == source
                flat[source * FIELDS + 2 * step + across] = slot
                where[piece] = (target, 2 * PIECES + 2 * step + across)
        for (source, which, piece), (chip, slot) in where.items():
            assert chip == combo[source][which]
            flat[chip * FIELDS + 2 * MAX_ROUNDS + (source * 2 + which) * PIECES + piece] = slot
        flat[4 * FIELDS] = max(len(rounds), BASE_ROUNDS) - BASE_ROUNDS
        rows[number] = flat.reshape(2, 128)
    return (index, rows)


def route_kernel(place_ref, matching_ref, index_ref, rows_ref, out_ref, row, dest, swap, sem):
    place = place_ref[0]
    chip = place // 2
    core = place % 2
    for position in range(8):
        dest[matching_ref[position]] = position // 2
    key = 0
    for at in range(4):
        first, second = dest[2 * at], dest[2 * at + 1]
        swap[at] = (first > second).astype(jnp.int32)
        if at < 3:
            lo, hi = jnp.minimum(first, second), jnp.maximum(first, second)
            key = key + 10**at * (lo * (7 - lo) // 2 + hi)
    copy = pltpu.make_async_copy(rows_ref.at[index_ref[key]], row, sem)
    copy.start()
    copy.wait()

    def field(flat):
        return row[flat // 128, flat % 128]

    def local_id(slot):
        owner = (slot // PIECES) ^ swap[chip]
        near = jnp.where(owner == core, 0, PIECES) + slot % PIECES
        return jnp.where(slot < 2 * PIECES, near, slot)

    for step in range(2 * MAX_ROUNDS):
        out_ref[step] = local_id(field(chip * FIELDS + step))
    layer = matching_ref[place]
    which = (layer % 2) ^ swap[layer // 2]
    base = chip * FIELDS + 2 * MAX_ROUNDS + (layer // 2 * 2 + which) * PIECES
    for piece in range(PIECES):
        out_ref[2 * MAX_ROUNDS + piece] = local_id(field(base + piece))
    out_ref[2 * MAX_ROUNDS + PIECES] = field(jnp.int32(4 * FIELDS))


def find_route(place, matching):
    index, rows = routing_tables()
    smem = pl.BlockSpec(memory_space=pltpu.SMEM)
    return pl.pallas_call(
        route_kernel,
        out_shape=jax.ShapeDtypeStruct((32,), jnp.int32),
        in_specs=[smem, smem, smem, pl.BlockSpec(memory_space=pl.ANY)],
        out_specs=smem,
        scratch_shapes=[
            pltpu.SMEM((2, 128), jnp.int32),
            pltpu.SMEM((8,), jnp.int32),
            pltpu.SMEM((4,), jnp.int32),
            pltpu.SemaphoreType.DMA,
        ],
        name="find_route",
    )(place, matching, jnp.asarray(index), jnp.asarray(rows))


def write_kernel(
    rows, first_of, place_ref, lengths_ref, cache_ref, fresh_ref, out_ref, held, wide, sem_in, sem_out
):
    first = first_of(place_ref[0])

    def copy_in(row):
        return pltpu.make_async_copy(cache_ref.at[0, first + row], held.at[row], sem_in.at[row])

    def copy_out(row):
        return pltpu.make_async_copy(held.at[row], out_ref.at[row], sem_out.at[row])

    for row in range(rows):
        copy_in(row).start()
    wide[...] = fresh_ref[0].astype(jnp.float32)
    for row in range(rows):
        copy_in(row).wait()
        length = lengths_ref[first + row]
        start = pl.multiple_of(length // 16 * 16, 16)
        tile = held[row, pl.ds(start, 16), :].astype(jnp.float32)
        fresh = wide[pl.ds(first + row, 1), :]
        places = lax.broadcasted_iota(jnp.int32, tile.shape, 0) + start
        tile = jnp.where(places == length, fresh, tile)
        held[row, pl.ds(start, 16), :] = tile.astype(held.dtype)
        copy_out(row).start()
    for row in range(rows):
        copy_out(row).wait()


def write_tokens(place, lengths, kv_cache, fresh, rows, first_of):
    smem = pl.BlockSpec(memory_space=pltpu.SMEM)
    shape = (rows,) + kv_cache.shape[2:]
    return pl.pallas_call(
        functools.partial(write_kernel, rows, first_of),
        out_shape=jax.ShapeDtypeStruct(shape, kv_cache.dtype),
        in_specs=[
            smem,
            smem,
            pl.BlockSpec(memory_space=pl.ANY),
            pl.BlockSpec(memory_space=pltpu.VMEM),
        ],
        out_specs=pl.BlockSpec(memory_space=pl.ANY),
        scratch_shapes=[
            pltpu.VMEM(shape, kv_cache.dtype),
            pltpu.VMEM(fresh.shape[1:], jnp.float32),
            pltpu.SemaphoreType.DMA((rows,)),
            pltpu.SemaphoreType.DMA((rows,)),
        ],
        name="write_tokens",
        cost_estimate=pl.CostEstimate(
            flops=2 * math.prod(shape), bytes_accessed=4 * math.prod(shape), transcendentals=0
        ),
    )(place, lengths, kv_cache, fresh)


def pick_kernel(step, n_near, n_after, ids_ref, *refs):
    refs = refs[n_after:]
    near = refs[:n_near]
    per = refs[0].shape[0] // PIECES
    passed = (len(refs) - n_near - 6) // 2
    relays = (refs[n_near : n_near + passed], refs[n_near + passed : n_near + 2 * passed])
    outs = refs[-6:-4]
    held = refs[-4:-2]
    sem_in, sem_out = refs[-2:]
    for way in range(2):
        wanted = ids_ref[2 * step + way]
        for number, ref in enumerate(near):

            @pl.when((wanted >= number * PIECES) & (wanted < (number + 1) * PIECES))
            def _(number=number, ref=ref, wanted=wanted, way=way):
                start = (wanted - number * PIECES) * per
                pltpu.make_async_copy(ref.at[pl.ds(start, per)], held[way], sem_in.at[way]).start()

        for past, ref in enumerate(relays[way]):

            @pl.when(wanted == 2 * PIECES + 2 * past + 1 - way)
            def _(ref=ref, way=way):
                pltpu.make_async_copy(ref, held[way], sem_in.at[way]).start()

    def copy_out(way):
        return pltpu.make_async_copy(held[way], outs[way], sem_out.at[way])

    for way in range(2):
        pltpu.make_async_copy(near[0].at[pl.ds(0, per)], held[way], sem_in.at[way]).wait()
        copy_out(way).start()
    for way in range(2):
        copy_out(way).wait()


def pick_pieces(ids, step, near, from_x, from_y, after=()):
    shape = (near[0].shape[0] // PIECES,) + near[0].shape[1:]
    held = pltpu.VMEM(shape, near[0].dtype)
    anywhere = pl.BlockSpec(memory_space=pl.ANY)
    operands = list(after) + list(near) + list(from_y) + list(from_x)
    one = jax.ShapeDtypeStruct(shape, near[0].dtype)
    return pl.pallas_call(
        functools.partial(pick_kernel, step, len(near), len(after)),
        out_shape=(one, one),
        in_specs=[pl.BlockSpec(memory_space=pltpu.SMEM)] + [anywhere] * len(operands),
        out_specs=(anywhere, anywhere),
        scratch_shapes=[
            held,
            held,
            pltpu.SemaphoreType.DMA((2,)),
            pltpu.SemaphoreType.DMA((2,)),
        ],
        name="pick_pieces",
        cost_estimate=pl.CostEstimate(
            flops=2 * math.prod(shape), bytes_accessed=8 * math.prod(shape), transcendentals=0
        ),
    )(ids, *operands)


def place_kernel(lo, hi, per, layout, place_ref, ids_ref, *refs):
    out_ref, held, sem_in, sem_out = refs[-4:]
    core = place_ref[0] % 2
    blocks = [
        (side, stream, piece)
        for stream in range(STREAMS)
        for side in range(2)
        for piece in range(PIECES)
    ]

    def row_of(side, stream, piece):
        half = core if side == 0 else 1 - core
        return half * (STREAMS * PIECES * per) + (stream * PIECES + piece) * per

    def move(at, side, stream, piece):
        wanted = ids_ref[2 * MAX_ROUNDS + piece]
        mine = (wanted >= lo) & (wanted < hi)
        for number in range(2):
            if lo < 2 * PIECES:

                @pl.when((wanted >= number * PIECES) & (wanted < (number + 1) * PIECES))
                def _(ref=refs[layout["near"][side][number][stream]]):
                    start = (wanted - number * PIECES) * per
                    pltpu.make_async_copy(
                        ref.at[pl.ds(start, per)], held.at[at], sem_in.at[at]
                    ).start()

        for slot, position in layout["far"][side][stream].items():
            if lo <= slot < hi:

                @pl.when(wanted == slot)
                def _(ref=refs[position]):
                    pltpu.make_async_copy(ref, held.at[at], sem_in.at[at]).start()

        return mine

    def copy_out(at, block):
        row = row_of(*block)
        return pltpu.make_async_copy(held.at[at], out_ref.at[0, pl.ds(row, per)], sem_out.at[at])

    mine = [move(at, *block) for at, block in enumerate(blocks)]
    for at, block in enumerate(blocks):

        @pl.when(mine[at])
        def _(at=at, block=block):
            pltpu.make_async_copy(
                out_ref.at[0, pl.ds(0, per)], held.at[at], sem_in.at[at]
            ).wait()
            copy_out(at, block).start()

    for at, block in enumerate(blocks):

        @pl.when(mine[at])
        def _(at=at, block=block):
            copy_out(at, block).wait()


def place_pieces(place, ids, lo, hi, near, far, result, out_shape, after=()):
    operands = []
    layout = {"near": [[[0, 0] for _ in range(2)] for _ in range(2)], "far": [[{}, {}], [{}, {}]]}

    def add(array):
        operands.append(array)
        return len(operands) - 1

    for side in range(2):
        for stream in range(STREAMS):
            if lo < 2 * PIECES:
                for owner in range(2):
                    layout["near"][side][owner][stream] = add(near[side][owner][stream])
            for slot, array in far[side][stream].items():
                if lo <= slot < hi:
                    layout["far"][side][stream][slot] = add(array)
    per = out_shape.shape[1] // (2 * STREAMS * PIECES)
    smem = pl.BlockSpec(memory_space=pltpu.SMEM)
    anywhere = pl.BlockSpec(memory_space=pl.ANY)
    operands += list(after)
    aliases = {}
    if result is not None:
        aliases = {2 + len(operands): 0}
        operands.append(result)
    count = 2 * STREAMS * PIECES
    return pl.pallas_call(
        functools.partial(place_kernel, lo, hi, per, layout),
        out_shape=out_shape,
        in_specs=[smem, smem] + [anywhere] * len(operands),
        out_specs=anywhere,
        scratch_shapes=[
            pltpu.VMEM((count, per) + out_shape.shape[2:], out_shape.dtype),
            pltpu.SemaphoreType.DMA((count,)),
            pltpu.SemaphoreType.DMA((count,)),
        ],
        input_output_aliases=aliases,
        name="place_pieces",
        cost_estimate=pl.CostEstimate(
            flops=math.prod(out_shape.shape),
            bytes_accessed=2 * math.prod(out_shape.shape),
            transcendentals=0,
        ),
    )(place, ids, *operands)


def attend_kernel(block, lengths_ref, q_ref, cache_ref, fresh_ref, *refs):
    out_ref = refs[-1]
    base = pl.program_id(0) * block
    slots = cache_ref.shape[2]
    per_key = q_ref.shape[1]
    scores = []
    for row in range(block):
        length = lengths_ref[base + row]
        key = cache_ref[0, row, :, :HEAD_SIZE]
        query = q_ref[row]
        fresh_key = fresh_ref[0, row : row + 1, :HEAD_SIZE]
        s = lax.dot_general(
            query, key, (((1,), (1,)), ((), ())), preferred_element_type=jnp.float32
        )
        new = jnp.sum(
            query.astype(jnp.float32) * fresh_key.astype(jnp.float32), axis=1, keepdims=True
        )
        spots = lax.broadcasted_iota(jnp.int32, (per_key, slots), 1)
        s = jnp.where(spots == length, new, s) / math.sqrt(HEAD_SIZE)
        scores.append(jnp.where(spots <= length, s, -1e30))
    scores = jnp.stack(scores)
    scores = jnp.exp(scores - jnp.max(scores, axis=-1, keepdims=True))
    weights = scores / jnp.sum(scores, axis=-1, keepdims=True)
    for row in range(block):
        length = lengths_ref[base + row]
        weight = weights[row].astype(jnp.bfloat16)
        wide = weight.astype(jnp.float32)
        spots = lax.broadcasted_iota(jnp.int32, (per_key, slots), 1)
        at_new = jnp.sum(jnp.where(spots == length, wide, 0.0), axis=1, keepdims=True)
        rest = jnp.where(spots == length, 0.0, wide).astype(jnp.bfloat16)
        value = cache_ref[0, row, :, HEAD_SIZE:]
        fresh_value = fresh_ref[0, row : row + 1, HEAD_SIZE:].astype(jnp.float32)
        total = jnp.dot(rest, value, preferred_element_type=jnp.float32)
        out_ref[row] = (total + at_new * fresh_value).astype(out_ref.dtype)


def attend(head, lengths, queries, kv_cache, fresh, after=()):
    block = 8
    rows, slots = kv_cache.shape[1:3]
    kv_heads = kv_cache.shape[3] // (2 * HEAD_SIZE)
    per_key = queries.shape[1] // kv_heads
    work = rows * per_key * slots * HEAD_SIZE
    return pl.pallas_call(
        functools.partial(attend_kernel, block),
        out_shape=jax.ShapeDtypeStruct((rows, per_key, HEAD_SIZE), jnp.bfloat16),
        grid_spec=pltpu.PrefetchScalarGridSpec(
            num_scalar_prefetch=1,
            grid=(rows // block,),
            in_specs=[
                pl.BlockSpec((block, per_key, HEAD_SIZE), lambda i, _: (i, head, 0)),
                pl.BlockSpec((1, block, slots, 2 * HEAD_SIZE), lambda i, _: (0, i, 0, head)),
                pl.BlockSpec((1, block, 2 * HEAD_SIZE), lambda i, _: (0, i, head)),
            ]
            + [pl.BlockSpec(memory_space=pl.ANY)] * len(after),
            out_specs=pl.BlockSpec((block, per_key, HEAD_SIZE), lambda i, _: (i, 0, 0)),
        ),
        name="attend",
        cost_estimate=pl.CostEstimate(
            flops=30 * work, bytes_accessed=rows * slots * 4 * HEAD_SIZE, transcendentals=0
        ),
    )(lengths, queries, kv_cache, fresh, *after)


def shift_pairs(size, shift):
    return [(at, (at + shift) % size) for at in range(size)]


def flip_pairs(size, mask):
    return [(at, at ^ mask) for at in range(size)]


def sum_over_tensor(value):
    size = lax.axis_size("tensor")
    total = value
    for shift in range(1, size):
        total = total + lax.ppermute(value, "tensor", shift_pairs(size, shift))
    return total


def scatter_sum(partial_value):
    size = lax.axis_size("tensor")
    parts = lax.all_to_all(partial_value, "tensor", split_axis=1, concat_axis=0, tiled=True)
    return jnp.sum(parts.reshape((size,) + (partial_value.shape[0], -1)), axis=0)


def norm_rows(stream, norm_gain):
    squares = sum_over_tensor(jnp.sum(stream * stream, axis=-1, keepdims=True))
    normed = stream * lax.rsqrt(squares / D + 1e-05) * norm_gain[0].astype(jnp.float32)
    return jnp.concatenate([stream.astype(jnp.bfloat16), normed.astype(jnp.bfloat16)], axis=1)


def spread_rows(matching, value):
    groups = lax.axis_size("section")
    folded = value.reshape((groups, value.shape[0] // groups) + value.shape[1:])
    spread = lax.all_to_all(folded, "section", split_axis=0, concat_axis=0, tiled=True)
    return jnp.take(spread, matching, axis=0, mode="clip")


def gather_rows(chosen, shape):
    landed = lax.all_to_all(chosen, "section", split_axis=0, concat_axis=0, tiled=True)
    return landed.reshape(shape)


def move_by_two_exchanges(matching, value):
    return gather_rows(spread_rows(matching, value), value.shape)


def on_any_section(
    matching, lengths, queries, kv_cache, incoming_key_value, residual, out_weight, norm_gain
):
    place = lax.axis_index("section").astype(jnp.int32).reshape(1)
    rows = kv_cache.shape[1]
    updated = write_tokens(
        place, lengths, kv_cache, incoming_key_value, rows, lambda _: 0
    )
    cache_out = move_by_two_exchanges(matching, updated)
    kv_heads = kv_cache.shape[3] // (2 * HEAD_SIZE)
    split_queries = queries.reshape(rows, -1, HEAD_SIZE)
    partial_value = 0.0
    depth = out_weight.shape[1] // kv_heads
    for head in range(kv_heads):
        attended = attend(head, lengths, split_queries, kv_cache, incoming_key_value)
        partial_value += jnp.dot(
            attended.reshape(rows, -1),
            out_weight[0, head * depth : (head + 1) * depth],
            preferred_element_type=jnp.float32,
        )
    stream = residual[0].astype(jnp.float32) + scatter_sum(partial_value)
    both = norm_rows(stream, norm_gain)
    both = move_by_two_exchanges(matching, both)
    width = both.shape[1] // 2
    return (cache_out[None], both[None, :, :width], both[None, :, width:])


def on_four_chips(
    matching, lengths, queries, kv_cache, incoming_key_value, residual, out_weight, norm_gain
):
    place = lax.axis_index("section").astype(jnp.int32).reshape(1)
    sections = lax.axis_size("section")
    across_core, across_x, across_y = (flip_pairs(sections, mask) for mask in (1, 2, 4))
    rows = kv_cache.shape[1]
    kv_heads = kv_cache.shape[3] // (2 * HEAD_SIZE)
    fresh = incoming_key_value
    part = rows // (2 * STREAMS)

    def swap(array):
        return lax.ppermute(array, "section", across_core)

    lent, kept, got = [], [], []
    for stream in range(STREAMS):
        lent.append(
            write_tokens(
                place, lengths, kv_cache, fresh, part,
                lambda p, s=stream: (1 - p % 2) * (rows // 2) + s * part,
            )
        )
        got.append(swap(lent[-1]))
    ids = find_route(place, matching)
    for stream in range(STREAMS):
        kept.append(
            write_tokens(
                place, lengths, kv_cache, fresh, part,
                lambda p, s=stream: p % 2 * (rows // 2) + s * part,
            )
        )

    from_x = [[] for _ in range(STREAMS)]
    from_y = [[] for _ in range(STREAMS)]
    far = [[{} for _ in range(STREAMS)] for _ in range(2)]

    def send(step, stream, from_x, from_y, kept, got, ids, after=()):
        out_x, out_y = pick_pieces(
            ids, step, (kept[stream], got[stream]), from_x[stream], from_y[stream], after
        )
        landed_x = lax.ppermute(out_x, "section", across_x)
        landed_y = lax.ppermute(out_y, "section", across_y)
        return ((landed_x, landed_y), out_x)

    def receive(step, stream, landed, from_x, from_y, far):
        for way, array in enumerate(landed):
            (from_x, from_y)[way][stream].append(array)
            slot = 2 * PIECES + 2 * step + way
            far[0][stream][slot] = array
            far[1][stream][slot] = swap(array)

    split_queries = queries.reshape(rows, -1, HEAD_SIZE)
    depth = out_weight.shape[1] // kv_heads
    work = {}

    def attend_head(head):
        work["attended"] = attend(
            head, lengths, split_queries, kv_cache, incoming_key_value, [work["sent"]]
        )
        return [work["attended"]]

    def project_head(head):
        product = jnp.dot(
            work["attended"].reshape(rows, -1),
            out_weight[0, head * depth : (head + 1) * depth],
            preferred_element_type=jnp.float32,
        )
        work["partial"] = product if head == 0 else work["partial"] + product
        return [work["partial"]]

    def add_parts():
        work["stream"] = residual[0].astype(jnp.float32) + scatter_sum(work["partial"])
        return [work["stream"]]

    def norm_stream():
        work["both"] = norm_rows(work["stream"], norm_gain)
        return [work["both"]]

    def spread_both():
        work["chosen"] = spread_rows(matching, work["both"])
        return [work["chosen"]]

    def gather_both():
        work["moved"] = gather_rows(work["chosen"], work["both"].shape)
        return [work["moved"]]

    chores = []
    for head in range(kv_heads):
        chores += [functools.partial(attend_head, head), functools.partial(project_head, head)]
    chores += [add_parts, norm_stream, spread_both, gather_both]
    after = []
    for step in range(BASE_ROUNDS):
        for stream in range(STREAMS):
            settled = [far[1][stream][s] for s in far[1][stream] if s < 2 * PIECES + 2 * step - 2]
            landed, work["sent"] = send(
                step, stream, from_x, from_y, kept, got, ids, after + settled[-2:]
            )
            receive(step, stream, landed, from_x, from_y, far)
            after = []
            if step + stream > 0 and chores:
                after = chores.pop(0)()
    for chore in chores:
        after = chore()
    lent_back = [swap(array) for array in kept]
    near = [[kept, got], [lent, lent_back]]
    both = work["moved"]
    out_shape = jax.ShapeDtypeStruct(kv_cache.shape, kv_cache.dtype)
    ready = 2 * PIECES + 2 * (BASE_ROUNDS - 1)
    result = place_pieces(place, ids, 0, ready, near, far, None, out_shape, after)

    def finish(extra, place, ids, kept, got, from_x, from_y, far, result):
        from_x, from_y = [list(a) for a in from_x], [list(a) for a in from_y]
        far = [[dict(a) for a in side] for side in far]
        lo = ready
        for step in range(BASE_ROUNDS, BASE_ROUNDS + extra):
            for stream in range(STREAMS):
                landed, _ = send(step, stream, from_x, from_y, kept, got, ids)
                receive(step, stream, landed, from_x, from_y, far)
        if extra:
            mid = 2 * PIECES + 2 * (BASE_ROUNDS + extra - 1)
            result = place_pieces(place, ids, lo, mid, None, far, result, out_shape)
            lo = mid
        top = 2 * PIECES + 2 * (BASE_ROUNDS + extra)
        return place_pieces(place, ids, lo, top, None, far, result, out_shape)

    late = [[{s: a for s, a in d.items() if s >= ready} for d in side] for side in far]
    cache_out = lax.switch(
        ids[2 * MAX_ROUNDS + PIECES],
        [functools.partial(finish, extra) for extra in range(MAX_ROUNDS - BASE_ROUNDS + 1)],
        place, ids, kept, got, from_x, from_y, late, result,
    )
    width = both.shape[1] // 2
    return (cache_out, both[None, :, :width], both[None, :, width:])


def solution(mesh):
    four_chips = mesh.shape["section"] == 8
    return jax.shard_map(
        on_four_chips if four_chips else on_any_section,
        mesh=mesh,
        in_specs=(
            P(),
            P(),
            P("section", None, "tensor"),
            P("section", None, None, "tensor"),
            P("section", None, "tensor"),
            P("section", None, "tensor"),
            P("section", "tensor", None),
            P("section", "tensor"),
        ),
        out_specs=(
            P("section", None, None, "tensor"),
            P("section", None, "tensor"),
            P("section", None, "tensor"),
        ),
        check_vma=False,
    )
```

```python
import functools
import itertools
import math
import random
import types

import jax
import jax.numpy as jnp
import numpy as np
from jax import lax
from jax.experimental import pallas as pl
from jax.experimental.pallas import tpu as pltpu
from jax.sharding import PartitionSpec as P


D = 8192
HEAD_SIZE = 128
SECTION = "section"
TENSOR = "tensor"
PIECES = 4
STREAMS = 2
MAX_ROUNDS = 8
BASE_ROUNDS = 5
FIELDS = 2 * MAX_ROUNDS + 8 * PIECES
RING = (0, 1, 3, 2)


def ring_path(source, target, clockwise):
    at = RING.index(source)
    hops = []
    while RING[at] != target:
        later = (at + (1 if clockwise else -1)) % 4
        hops.append((RING[at], RING[later]))
        at = later
    return hops


def demand_classes():
    pairs = [(a, b) for a in range(4) for b in range(a, 4)]
    return [
        combo
        for combo in itertools.product(pairs, repeat=4)
        if all(sum(pair.count(chip) for pair in combo) == 2 for chip in range(4))
    ]


def split_directions(items, rng):
    share = {}
    for source, which, target in items:
        gap = (RING.index(target) - RING.index(source)) % 4
        share[(source, which)] = {1: PIECES, 2: PIECES // 2, 3: 0}[gap]

    def cost():
        load = {}
        for source, which, target in items:
            count = share[(source, which)]
            for hop in ring_path(source, target, True):
                load[hop] = load.get(hop, 0) + count
            for hop in ring_path(source, target, False):
                load[hop] = load.get(hop, 0) + PIECES - count
        return (max(load.values(), default=0), sum(v * v for v in load.values()))

    keys = list(share)
    single = [((key, step),) for key in keys for step in (1, -1, 2, -2)]
    double = [
        ((key, a), (other, b))
        for key, other in itertools.combinations(keys, 2)
        for a in (1, -1)
        for b in (1, -1)
    ]
    best = cost()
    improved = True
    while improved:
        improved = False
        moves = single + double
        rng.shuffle(moves)
        for move in moves:
            if any(not 0 <= share[key] + step <= PIECES for key, step in move):
                continue
            for key, step in move:
                share[key] += step
            now = cost()
            if now < best:
                best = now
                improved = True
                break
            for key, step in move:
                share[key] -= step
    return (share, best[0])


def schedule_rounds(items, share, rng, noise):
    pieces = []
    for source, which, target in items:
        for number in range(PIECES):
            hops = ring_path(source, target, number < share[(source, which)])
            pieces.append([hops, 0, 0, (source, which, number)])
    rounds = []
    while any(piece[1] < len(piece[0]) for piece in pieces):
        taken = {}
        for piece in sorted(
            pieces, key=lambda piece: piece[1] - len(piece[0]) + noise * rng.random()
        ):
            if piece[1] < len(piece[0]) and piece[2] <= len(rounds):
                taken.setdefault(piece[0][piece[1]], piece)
        for piece in taken.values():
            piece[1] += 1
            piece[2] = len(rounds) + 1
        rounds.append({hop: piece[3] for hop, piece in taken.items()})
    return rounds


def solve_class(combo, tries=60):
    rng = random.Random(7)
    items = [
        (source, which, target)
        for source, pair in enumerate(combo)
        for which, target in enumerate(pair)
        if source != target
    ]
    best = None
    for attempt in range(tries):
        if attempt % 5 == 0:
            share, bound = split_directions(items, rng)
        rounds = schedule_rounds(items, share, rng, (0.5, 1.0, 1.0, 1.5, 2.5)[attempt % 5])
        if best is None or len(rounds) < len(best):
            best = rounds
        if len(best) <= bound:
            break
    assert len(best) <= MAX_ROUNDS
    return best


@functools.cache
def routing_tables():
    classes = demand_classes()
    index = np.zeros((1000,), np.int32)
    rows = np.zeros((len(classes), 2, 128), np.int32)
    for number, combo in enumerate(classes):
        ids = [lo * (7 - lo) // 2 + hi for lo, hi in combo]
        index[ids[0] + 10 * ids[1] + 100 * ids[2]] = number
        where = {
            (chip, which, piece): (chip, which * PIECES + piece)
            for chip in range(4)
            for which in range(2)
            for piece in range(PIECES)
        }
        flat = np.zeros((256,), np.int32)
        rounds = solve_class(combo)
        for step, taken in enumerate(rounds):
            for (source, target), piece in taken.items():
                across = 0 if source ^ target == 1 else 1
                chip, slot = where[piece]
                assert chip == source
                flat[source * FIELDS + 2 * step + across] = slot
                where[piece] = (target, 2 * PIECES + 2 * step + across)
        for (source, which, piece), (chip, slot) in where.items():
            assert chip == combo[source][which]
            flat[chip * FIELDS + 2 * MAX_ROUNDS + (source * 2 + which) * PIECES + piece] = slot
        flat[4 * FIELDS] = max(len(rounds), BASE_ROUNDS) - BASE_ROUNDS
        rows[number] = flat.reshape(2, 128)
    return (index, rows)


def route_kernel(place_ref, matching_ref, index_ref, rows_ref, out_ref, row, dest, swap, sem):
    place = place_ref[0]
    chip = place // 2
    core = place % 2
    for position in range(8):
        dest[matching_ref[position]] = position // 2
    key = 0
    for at in range(4):
        first, second = dest[2 * at], dest[2 * at + 1]
        swap[at] = (first > second).astype(jnp.int32)
        if at < 3:
            lo, hi = jnp.minimum(first, second), jnp.maximum(first, second)
            key = key + 10**at * (lo * (7 - lo) // 2 + hi)
    copy = pltpu.make_async_copy(rows_ref.at[index_ref[key]], row, sem)
    copy.start()
    copy.wait()

    def field(flat):
        return row[flat // 128, flat % 128]

    def local_id(slot):
        owner = (slot // PIECES) ^ swap[chip]
        near = jnp.where(owner == core, 0, PIECES) + slot % PIECES
        return jnp.where(slot < 2 * PIECES, near, slot)

    for step in range(2 * MAX_ROUNDS):
        out_ref[step] = local_id(field(chip * FIELDS + step))
    layer = matching_ref[place]
    which = (layer % 2) ^ swap[layer // 2]
    base = chip * FIELDS + 2 * MAX_ROUNDS + (layer // 2 * 2 + which) * PIECES
    for piece in range(PIECES):
        out_ref[2 * MAX_ROUNDS + piece] = local_id(field(base + piece))
    out_ref[2 * MAX_ROUNDS + PIECES] = field(jnp.int32(4 * FIELDS))


def find_route(place, matching):
    index, rows = routing_tables()
    smem = pl.BlockSpec(memory_space=pltpu.SMEM)
    return pl.pallas_call(
        route_kernel,
        out_shape=jax.ShapeDtypeStruct((32,), jnp.int32),
        in_specs=[smem, smem, smem, pl.BlockSpec(memory_space=pl.ANY)],
        out_specs=smem,
        scratch_shapes=[
            pltpu.SMEM((2, 128), jnp.int32),
            pltpu.SMEM((8,), jnp.int32),
            pltpu.SMEM((4,), jnp.int32),
            pltpu.SemaphoreType.DMA,
        ],
    )(place, matching, jnp.asarray(index), jnp.asarray(rows))


def write_kernel(
    rows, first_of, place_ref, lengths_ref, cache_ref, fresh_ref, *refs
):
    out_ref, held, wide, sem_in, sem_out = refs[-5:]
    first = first_of(place_ref[0])

    def copy_in(row):
        return pltpu.make_async_copy(cache_ref.at[0, first + row], held.at[row], sem_in.at[row])

    def copy_out(row):
        return pltpu.make_async_copy(held.at[row], out_ref.at[row], sem_out.at[row])

    for row in range(rows):
        copy_in(row).start()
    wide[...] = fresh_ref[0].astype(jnp.float32)
    for row in range(rows):
        copy_in(row).wait()
        length = lengths_ref[first + row]
        start = pl.multiple_of(length // 16 * 16, 16)
        tile = held[row, pl.ds(start, 16), :].astype(jnp.float32)
        fresh = wide[pl.ds(first + row, 1), :]
        places = lax.broadcasted_iota(jnp.int32, tile.shape, 0) + start
        tile = jnp.where(places == length, fresh, tile)
        held[row, pl.ds(start, 16), :] = tile.astype(held.dtype)
        copy_out(row).start()
    for row in range(rows):
        copy_out(row).wait()


def write_tokens(place, lengths, kv_cache, fresh, rows, first_of, after=()):
    smem = pl.BlockSpec(memory_space=pltpu.SMEM)
    shape = (rows,) + kv_cache.shape[2:]
    return pl.pallas_call(
        functools.partial(write_kernel, rows, first_of),
        out_shape=jax.ShapeDtypeStruct(shape, kv_cache.dtype),
        in_specs=[
            smem,
            smem,
            pl.BlockSpec(memory_space=pl.ANY),
            pl.BlockSpec(memory_space=pltpu.VMEM),
        ]
        + [pl.BlockSpec(memory_space=pl.ANY)] * len(after),
        out_specs=pl.BlockSpec(memory_space=pl.ANY),
        scratch_shapes=[
            pltpu.VMEM(shape, kv_cache.dtype),
            pltpu.VMEM(fresh.shape[1:], jnp.float32),
            pltpu.SemaphoreType.DMA((rows,)),
            pltpu.SemaphoreType.DMA((rows,)),
        ],
        cost_estimate=pl.CostEstimate(
            flops=2 * math.prod(shape), bytes_accessed=4 * math.prod(shape), transcendentals=0
        ),
    )(place, lengths, kv_cache, fresh, *after)


def pick_kernel(step, n_near, n_after, ids_ref, *refs):
    outs, sems = refs[-3:-1], refs[-1]
    refs = refs[n_after:-3]
    near = refs[:n_near]
    passed = (len(refs) - n_near) // 2
    relays = (refs[n_near : n_near + passed], refs[n_near + passed :])
    per = outs[0].shape[0]
    for way in range(2):
        wanted = ids_ref[2 * step + way]
        for number, ref in enumerate(near):

            @pl.when((wanted >= number * PIECES) & (wanted < (number + 1) * PIECES))
            def _(number=number, ref=ref, wanted=wanted, way=way):
                start = (wanted - number * PIECES) * per
                pltpu.make_async_copy(ref.at[pl.ds(start, per)], outs[way], sems.at[way]).start()

        for past, ref in enumerate(relays[way]):

            @pl.when(wanted == 2 * PIECES + 2 * past + 1 - way)
            def _(ref=ref, way=way):
                pltpu.make_async_copy(ref, outs[way], sems.at[way]).start()

    for way in range(2):
        pltpu.make_async_copy(near[0].at[pl.ds(0, per)], outs[way], sems.at[way]).wait()


def pick_pieces(ids, step, near, from_x, from_y, after=()):
    shape = (near[0].shape[0] // PIECES,) + near[0].shape[1:]
    anywhere = pl.BlockSpec(memory_space=pl.ANY)
    operands = list(after) + list(near) + list(from_y) + list(from_x)
    one = pltpu.VMEM(shape, near[0].dtype)
    vmem = pl.BlockSpec(memory_space=pltpu.VMEM)
    return pl.pallas_call(
        functools.partial(pick_kernel, step, len(near), len(after)),
        out_shape=(one, one),
        in_specs=[pl.BlockSpec(memory_space=pltpu.SMEM)] + [anywhere] * len(operands),
        out_specs=(vmem, vmem),
        scratch_shapes=[pltpu.SemaphoreType.DMA((2,))],
        cost_estimate=pl.CostEstimate(
            flops=2 * math.prod(shape), bytes_accessed=8 * math.prod(shape), transcendentals=0
        ),
    )(ids, *operands)


def place_kernel(lo, hi, per, near_at, far_at, place_ref, ids_ref, *refs):
    out_ref, held, sem_in, sem_out = refs[-4:]
    core = place_ref[0] % 2
    blocks = [
        (side, stream, piece)
        for stream in range(STREAMS)
        for side in range(2)
        for piece in range(PIECES)
    ]

    def row_of(side, stream, piece):
        half = core if side == 0 else 1 - core
        return half * (STREAMS * PIECES * per) + (stream * PIECES + piece) * per

    def move(at, side, stream, piece):
        wanted = ids_ref[2 * MAX_ROUNDS + piece]
        mine = (wanted >= lo) & (wanted < hi)
        for number in range(2):
            if lo < 2 * PIECES:

                @pl.when((wanted >= number * PIECES) & (wanted < (number + 1) * PIECES))
                def _(ref=refs[near_at[side][number][stream]]):
                    start = (wanted - number * PIECES) * per
                    pltpu.make_async_copy(
                        ref.at[pl.ds(start, per)], held.at[at], sem_in.at[at]
                    ).start()

        for slot, position in far_at[side][stream].items():
            if lo <= slot < hi:

                @pl.when(wanted == slot)
                def _(ref=refs[position]):
                    pltpu.make_async_copy(ref, held.at[at], sem_in.at[at]).start()

        return mine

    def copy_out(at, block):
        row = row_of(*block)
        return pltpu.make_async_copy(held.at[at], out_ref.at[0, pl.ds(row, per)], sem_out.at[at])

    mine = [move(at, *block) for at, block in enumerate(blocks)]
    for at, block in enumerate(blocks):

        @pl.when(mine[at])
        def _(at=at, block=block):
            pltpu.make_async_copy(
                out_ref.at[0, pl.ds(0, per)], held.at[at], sem_in.at[at]
            ).wait()
            copy_out(at, block).start()

    for at, block in enumerate(blocks):

        @pl.when(mine[at])
        def _(at=at, block=block):
            copy_out(at, block).wait()


def place_pieces(place, ids, lo, hi, near, far, result, out_shape, after=()):
    operands = []
    near_at = [[[0, 0] for _ in range(2)] for _ in range(2)]
    far_at = [[{}, {}], [{}, {}]]

    def add(array):
        operands.append(array)
        return len(operands) - 1

    for side in range(2):
        for stream in range(STREAMS):
            if lo < 2 * PIECES:
                for owner in range(2):
                    near_at[side][owner][stream] = add(near[side][owner][stream])
            for slot, array in far[side][stream].items():
                if lo <= slot < hi:
                    far_at[side][stream][slot] = add(array)
    per = out_shape.shape[1] // (2 * STREAMS * PIECES)
    smem = pl.BlockSpec(memory_space=pltpu.SMEM)
    anywhere = pl.BlockSpec(memory_space=pl.ANY)
    operands += list(after)
    aliases = {}
    if result is not None:
        aliases = {2 + len(operands): 0}
        operands.append(result)
    count = 2 * STREAMS * PIECES
    return pl.pallas_call(
        functools.partial(place_kernel, lo, hi, per, near_at, far_at),
        out_shape=out_shape,
        in_specs=[smem, smem] + [anywhere] * len(operands),
        out_specs=anywhere,
        scratch_shapes=[
            pltpu.VMEM((count, per) + out_shape.shape[2:], out_shape.dtype),
            pltpu.SemaphoreType.DMA((count,)),
            pltpu.SemaphoreType.DMA((count,)),
        ],
        input_output_aliases=aliases,
        cost_estimate=pl.CostEstimate(
            flops=math.prod(out_shape.shape),
            bytes_accessed=2 * math.prod(out_shape.shape),
            transcendentals=0,
        ),
    )(place, ids, *operands)


def attend_kernel(block, lengths_ref, q_ref, cache_ref, fresh_ref, *refs):
    out_ref = refs[-1]
    base = pl.program_id(0) * block
    slots = cache_ref.shape[2]
    per_key = q_ref.shape[1]
    scores = []
    for row in range(block):
        length = lengths_ref[base + row]
        key = cache_ref[0, row, :, :HEAD_SIZE]
        query = q_ref[row]
        fresh_key = fresh_ref[0, row : row + 1, :HEAD_SIZE]
        s = lax.dot_general(
            query, key, (((1,), (1,)), ((), ())), preferred_element_type=jnp.float32
        )
        new = jnp.sum(
            query.astype(jnp.float32) * fresh_key.astype(jnp.float32), axis=1, keepdims=True
        )
        spots = lax.broadcasted_iota(jnp.int32, (per_key, slots), 1)
        s = jnp.where(spots == length, new, s) / math.sqrt(HEAD_SIZE)
        scores.append(jnp.where(spots <= length, s, -1e30))
    scores = jnp.stack(scores)
    scores = jnp.exp(scores - jnp.max(scores, axis=-1, keepdims=True))
    weights = scores / jnp.sum(scores, axis=-1, keepdims=True)
    for row in range(block):
        length = lengths_ref[base + row]
        weight = weights[row].astype(jnp.bfloat16)
        wide = weight.astype(jnp.float32)
        spots = lax.broadcasted_iota(jnp.int32, (per_key, slots), 1)
        at_new = jnp.sum(jnp.where(spots == length, wide, 0.0), axis=1, keepdims=True)
        rest = jnp.where(spots == length, 0.0, wide).astype(jnp.bfloat16)
        value = cache_ref[0, row, :, HEAD_SIZE:]
        fresh_value = fresh_ref[0, row : row + 1, HEAD_SIZE:].astype(jnp.float32)
        total = jnp.dot(rest, value, preferred_element_type=jnp.float32)
        out_ref[row] = (total + at_new * fresh_value).astype(out_ref.dtype)


def attend(head, lengths, queries, kv_cache, fresh, after=()):
    block = 8
    rows, slots = kv_cache.shape[1:3]
    kv_heads = kv_cache.shape[3] // (2 * HEAD_SIZE)
    per_key = queries.shape[1] // kv_heads
    work = rows * per_key * slots * HEAD_SIZE
    return pl.pallas_call(
        functools.partial(attend_kernel, block),
        out_shape=jax.ShapeDtypeStruct((rows, per_key, HEAD_SIZE), jnp.bfloat16),
        grid_spec=pltpu.PrefetchScalarGridSpec(
            num_scalar_prefetch=1,
            grid=(rows // block,),
            in_specs=[
                pl.BlockSpec((block, per_key, HEAD_SIZE), lambda i, _: (i, head, 0)),
                pl.BlockSpec((1, block, slots, 2 * HEAD_SIZE), lambda i, _: (0, i, 0, head)),
                pl.BlockSpec((1, block, 2 * HEAD_SIZE), lambda i, _: (0, i, head)),
            ]
            + [pl.BlockSpec(memory_space=pl.ANY)] * len(after),
            out_specs=pl.BlockSpec((block, per_key, HEAD_SIZE), lambda i, _: (i, 0, 0)),
        ),
        cost_estimate=pl.CostEstimate(
            flops=30 * work, bytes_accessed=rows * slots * 4 * HEAD_SIZE, transcendentals=0
        ),
    )(lengths, queries, kv_cache, fresh, *after)


def add_kernel(parts_ref, residual_ref, stream_ref, squares_ref):
    total = residual_ref[0].astype(jnp.float32)
    added = parts_ref[0]
    for part in range(1, parts_ref.shape[0]):
        added = added + parts_ref[part]
    total = total + added
    stream_ref[...] = total
    squares = jnp.sum(total * total, axis=-1, keepdims=True)
    squares_ref[...] = jnp.broadcast_to(squares, squares_ref.shape)


def add_parts_kernel(parts, residual):
    rows, width = residual.shape[1:]
    return pl.pallas_call(
        add_kernel,
        out_shape=(
            jax.ShapeDtypeStruct((rows, width), jnp.float32),
            jax.ShapeDtypeStruct((rows, 128), jnp.float32),
        ),
        cost_estimate=pl.CostEstimate(
            flops=8 * parts.size, bytes_accessed=4 * parts.size, transcendentals=0
        ),
    )(parts, residual)


def norm_kernel(groups, stream_ref, gain_ref, *refs):
    both_ref = refs[-1]
    stream = stream_ref[...]
    squares = refs[0][:, :1]
    for ref in refs[1:-1]:
        squares = squares + ref[:, :1]
    normed = stream * lax.rsqrt(squares / D + 1e-05) * gain_ref[...].astype(jnp.float32)
    per = stream.shape[0] // groups
    for group in range(groups):
        chunk = slice(group * per, (group + 1) * per)
        pair = jnp.concatenate([stream[chunk], normed[chunk]], axis=0)
        both_ref[group] = pair.astype(both_ref.dtype)


def norm_both(groups, stream, norm_gain, squares):
    rows, width = stream.shape
    return pl.pallas_call(
        functools.partial(norm_kernel, groups),
        out_shape=jax.ShapeDtypeStruct((groups, 2 * rows // groups, width), jnp.bfloat16),
        cost_estimate=pl.CostEstimate(
            flops=60 * stream.size, bytes_accessed=8 * stream.size, transcendentals=0
        ),
    )(stream, norm_gain, *squares)


def part_kernel(landed_ref, stream_ref, normed_ref):
    groups, double = landed_ref.shape[:2]
    per = double // 2
    landed = landed_ref[...].astype(jnp.float32)
    for way, ref in enumerate((stream_ref, normed_ref)):
        chunks = [landed[group, way * per : (way + 1) * per] for group in range(groups)]
        ref[0] = jnp.concatenate(chunks, axis=0).astype(ref.dtype)


def part_both(landed):
    groups, double, width = landed.shape
    one = jax.ShapeDtypeStruct((1, groups * double // 2, width), landed.dtype)
    return pl.pallas_call(part_kernel, out_shape=(one, one))(landed)


def shift_pairs(size, shift):
    return [(at, (at + shift) % size) for at in range(size)]


def flip_pairs(size, mask):
    return [(at, at ^ mask) for at in range(size)]


def sum_over_tensor(value):
    size = lax.axis_size(TENSOR)
    total = value
    for shift in range(1, size):
        total = total + lax.ppermute(value, TENSOR, shift_pairs(size, shift))
    return total


def scatter_sum(partial_value):
    size = lax.axis_size(TENSOR)
    parts = lax.all_to_all(partial_value, TENSOR, split_axis=1, concat_axis=0, tiled=True)
    return jnp.sum(parts.reshape((size,) + (partial_value.shape[0], -1)), axis=0)


def norm_rows(stream, norm_gain):
    squares = sum_over_tensor(jnp.sum(stream * stream, axis=-1, keepdims=True))
    normed = stream * lax.rsqrt(squares / D + 1e-05) * norm_gain[0].astype(jnp.float32)
    return jnp.concatenate([stream.astype(jnp.bfloat16), normed.astype(jnp.bfloat16)], axis=1)


def spread_rows(matching, value):
    groups = lax.axis_size(SECTION)
    folded = value.reshape((groups, value.shape[0] // groups) + value.shape[1:])
    spread = lax.all_to_all(folded, SECTION, split_axis=0, concat_axis=0, tiled=True)
    return jnp.take(spread, matching, axis=0, mode="clip")


def gather_rows(chosen, shape):
    landed = lax.all_to_all(chosen, SECTION, split_axis=0, concat_axis=0, tiled=True)
    return landed.reshape(shape)


def move_by_two_exchanges(matching, value):
    return gather_rows(spread_rows(matching, value), value.shape)


def on_any_section(
    matching, lengths, queries, kv_cache, incoming_key_value, residual, out_weight, norm_gain
):
    place = lax.axis_index(SECTION).astype(jnp.int32).reshape(1)
    rows = kv_cache.shape[1]
    updated = write_tokens(
        place, lengths, kv_cache, incoming_key_value, rows, lambda _: 0
    )
    cache_out = move_by_two_exchanges(matching, updated)
    kv_heads = kv_cache.shape[3] // (2 * HEAD_SIZE)
    split_queries = queries.reshape(rows, -1, HEAD_SIZE)
    partial_value = 0.0
    depth = out_weight.shape[1] // kv_heads
    for head in range(kv_heads):
        attended = attend(head, lengths, split_queries, kv_cache, incoming_key_value)
        partial_value += jnp.dot(
            attended.reshape(rows, -1),
            out_weight[0, head * depth : (head + 1) * depth],
            preferred_element_type=jnp.float32,
        )
    stream = residual[0].astype(jnp.float32) + scatter_sum(partial_value)
    both = norm_rows(stream, norm_gain)
    both = move_by_two_exchanges(matching, both)
    width = both.shape[1] // 2
    return (cache_out[None], both[None, :, :width], both[None, :, width:])


def on_four_chips(
    matching, lengths, queries, kv_cache, incoming_key_value, residual, out_weight, norm_gain
):
    place = lax.axis_index(SECTION).astype(jnp.int32).reshape(1)
    sections = lax.axis_size(SECTION)
    across_core, across_x, across_y = (flip_pairs(sections, mask) for mask in (1, 2, 4))
    rows = kv_cache.shape[1]
    kv_heads = kv_cache.shape[3] // (2 * HEAD_SIZE)
    fresh = incoming_key_value
    part = rows // (2 * STREAMS)

    def swap(array):
        return lax.ppermute(array, SECTION, across_core)

    lent, kept, got = [], [], []

    def share(stream, after=()):
        lent.append(
            write_tokens(
                place, lengths, kv_cache, fresh, part,
                lambda p: (1 - p % 2) * (rows // 2) + stream * part, after,
            )
        )
        got.append(swap(lent[-1]))
        kept.append(
            write_tokens(
                place, lengths, kv_cache, fresh, part,
                lambda p: p % 2 * (rows // 2) + stream * part, [lent[-1]],
            )
        )

    ids = find_route(place, matching)

    from_x = [[] for _ in range(STREAMS)]
    from_y = [[] for _ in range(STREAMS)]
    far = [[{} for _ in range(STREAMS)] for _ in range(2)]

    def send(step, stream, from_x, from_y, kept, got, ids, after=()):
        out_x, out_y = pick_pieces(
            ids, step, (kept[stream], got[stream]), from_x[stream], from_y[stream], after
        )
        landed_x = lax.ppermute(out_x, SECTION, across_x)
        landed_y = lax.ppermute(out_y, SECTION, across_y)
        return ((landed_x, landed_y), out_x)

    def receive(step, stream, landed, from_x, from_y, far):
        for way, array in enumerate(landed):
            (from_x, from_y)[way][stream].append(array)
            slot = 2 * PIECES + 2 * step + way
            far[0][stream][slot] = array
            far[1][stream][slot] = swap(array)

    split_queries = queries.reshape(rows, -1, HEAD_SIZE)
    depth = out_weight.shape[1] // kv_heads
    work = types.SimpleNamespace(sent=None)

    def attend_head(head):
        work.attended = attend(
            head, lengths, split_queries, kv_cache, incoming_key_value, [work.sent]
        )
        return [work.attended]

    def project_head(head):
        product = jnp.dot(
            work.attended.reshape(rows, -1),
            out_weight[0, head * depth : (head + 1) * depth],
            preferred_element_type=jnp.float32,
        )
        work.partial = product if head == 0 else work.partial + product
        return [work.partial]

    def add_parts():
        parts = lax.all_to_all(
            work.partial, TENSOR, split_axis=1, concat_axis=0, tiled=True
        )
        parts = parts.reshape(lax.axis_size(TENSOR), rows, -1)
        work.stream, squares = add_parts_kernel(parts, residual)
        tensors = lax.axis_size(TENSOR)
        work.squares = [squares] + [
            lax.ppermute(squares, TENSOR, shift_pairs(tensors, shift))
            for shift in range(1, tensors)
        ]
        return [work.stream]

    def norm_stream():
        work.both = norm_both(sections, work.stream, norm_gain, work.squares)
        return [work.both]

    def move_both():
        spread = lax.all_to_all(work.both, SECTION, split_axis=0, concat_axis=0, tiled=True)
        chosen = jnp.take(spread, matching, axis=0, mode="clip")
        work.landed = lax.all_to_all(
            chosen, SECTION, split_axis=0, concat_axis=0, tiled=True
        )
        return [chosen]

    def split_both():
        work.outs = part_both(work.landed)
        return [work.sent]

    chores = []
    for head in range(kv_heads):
        chores += [functools.partial(attend_head, head), functools.partial(project_head, head)]
    out_shape = jax.ShapeDtypeStruct(kv_cache.shape, kv_cache.dtype)
    early = 2 * PIECES + 4

    def place_early():
        lent_back = [swap(array) for array in kept]
        near = [[kept, got], [lent, lent_back]]
        work.result = place_pieces(place, ids, 0, early, near, far, None, out_shape, [work.sent])
        return add_parts()

    chores += [None, place_early, norm_stream, move_both, split_both]
    after = []
    for step in range(BASE_ROUNDS):
        for stream in range(STREAMS):
            settled = [far[1][stream][s] for s in far[1][stream] if s < 2 * PIECES + 2 * step - 2]
            if step == 0:
                share(stream, [work.sent] if stream else [])
            landed, work.sent = send(
                step, stream, from_x, from_y, kept, got, ids, after + settled[-2:]
            )
            receive(step, stream, landed, from_x, from_y, far)
            chore = chores.pop(0) if step + stream > 0 and chores else None
            after = chore() if chore else []
    for chore in filter(None, chores):
        after = chore()
    stream_out, normed_out = work.outs
    ready = 2 * PIECES + 2 * (BASE_ROUNDS - 1)
    result = place_pieces(
        place, ids, early, ready, None, far, work.result, out_shape, after
    )

    def finish(extra, place, ids, kept, got, from_x, from_y, far, result):
        from_x, from_y = [list(a) for a in from_x], [list(a) for a in from_y]
        far = [[dict(a) for a in side] for side in far]
        lo = ready
        for step in range(BASE_ROUNDS, BASE_ROUNDS + extra):
            for stream in range(STREAMS):
                landed, _ = send(step, stream, from_x, from_y, kept, got, ids)
                receive(step, stream, landed, from_x, from_y, far)
        if extra:
            mid = 2 * PIECES + 2 * (BASE_ROUNDS + extra - 1)
            result = place_pieces(place, ids, lo, mid, None, far, result, out_shape)
            lo = mid
        top = 2 * PIECES + 2 * (BASE_ROUNDS + extra)
        return place_pieces(place, ids, lo, top, None, far, result, out_shape)

    late = [[{s: a for s, a in d.items() if s >= ready} for d in side] for side in far]
    cache_out = lax.switch(
        ids[2 * MAX_ROUNDS + PIECES],
        [functools.partial(finish, extra) for extra in range(MAX_ROUNDS - BASE_ROUNDS + 1)],
        place, ids, kept, got, from_x, from_y, late, result,
    )
    return (cache_out, stream_out, normed_out)


def solution(mesh):
    four_chips = mesh.shape[SECTION] == 8
    return jax.shard_map(
        on_four_chips if four_chips else on_any_section,
        mesh=mesh,
        in_specs=(
            P(),
            P(),
            P(SECTION, None, TENSOR),
            P(SECTION, None, None, TENSOR),
            P(SECTION, None, TENSOR),
            P(SECTION, None, TENSOR),
            P(SECTION, TENSOR, None),
            P(SECTION, TENSOR),
        ),
        out_specs=(
            P(SECTION, None, None, TENSOR),
            P(SECTION, None, TENSOR),
            P(SECTION, None, TENSOR),
        ),
        check_vma=False,
    )
```

```python
import functools
import itertools
import math
import random
import types

import jax
import jax.numpy as jnp
import numpy as np
from jax import lax
from jax.experimental import pallas as pl
from jax.experimental.pallas import tpu as pltpu
from jax.sharding import PartitionSpec as P


D = 8192
HEAD_SIZE = 128
SECTION = "section"
TENSOR = "tensor"
PIECES = 4
STREAMS = 2
MAX_ROUNDS = 8
BASE_ROUNDS = 5
FIELDS = 2 * MAX_ROUNDS + 8 * PIECES
RING = (0, 1, 3, 2)


def ring_path(source, target, clockwise):
    at = RING.index(source)
    hops = []
    while RING[at] != target:
        later = (at + (1 if clockwise else -1)) % 4
        hops.append((RING[at], RING[later]))
        at = later
    return hops


def demand_classes():
    pairs = [(a, b) for a in range(4) for b in range(a, 4)]
    return [
        combo
        for combo in itertools.product(pairs, repeat=4)
        if all(sum(pair.count(chip) for pair in combo) == 2 for chip in range(4))
    ]


def split_directions(items, rng):
    share = {}
    for source, which, target in items:
        gap = (RING.index(target) - RING.index(source)) % 4
        share[(source, which)] = {1: PIECES, 2: PIECES // 2, 3: 0}[gap]

    def cost():
        load = {}
        for source, which, target in items:
            count = share[(source, which)]
            for hop in ring_path(source, target, True):
                load[hop] = load.get(hop, 0) + count
            for hop in ring_path(source, target, False):
                load[hop] = load.get(hop, 0) + PIECES - count
        return (max(load.values(), default=0), sum(v * v for v in load.values()))

    keys = list(share)
    single = [((key, step),) for key in keys for step in (1, -1, 2, -2)]
    double = [
        ((key, a), (other, b))
        for key, other in itertools.combinations(keys, 2)
        for a in (1, -1)
        for b in (1, -1)
    ]
    best = cost()
    improved = True
    while improved:
        improved = False
        moves = single + double
        rng.shuffle(moves)
        for move in moves:
            if any(not 0 <= share[key] + step <= PIECES for key, step in move):
                continue
            for key, step in move:
                share[key] += step
            now = cost()
            if now < best:
                best = now
                improved = True
                break
            for key, step in move:
                share[key] -= step
    return (share, best[0])


def schedule_rounds(items, share, rng, noise):
    pieces = []
    for source, which, target in items:
        for number in range(PIECES):
            hops = ring_path(source, target, number < share[(source, which)])
            pieces.append([hops, 0, 0, (source, which, number)])
    rounds = []
    while any(piece[1] < len(piece[0]) for piece in pieces):
        taken = {}
        for piece in sorted(
            pieces, key=lambda piece: piece[1] - len(piece[0]) + noise * rng.random()
        ):
            if piece[1] < len(piece[0]) and piece[2] <= len(rounds):
                taken.setdefault(piece[0][piece[1]], piece)
        for piece in taken.values():
            piece[1] += 1
            piece[2] = len(rounds) + 1
        rounds.append({hop: piece[3] for hop, piece in taken.items()})
    return rounds


def solve_class(combo, tries=60):
    rng = random.Random(7)
    items = [
        (source, which, target)
        for source, pair in enumerate(combo)
        for which, target in enumerate(pair)
        if source != target
    ]
    best = None
    for attempt in range(tries):
        if attempt % 5 == 0:
            share, bound = split_directions(items, rng)
        rounds = schedule_rounds(items, share, rng, (0.5, 1.0, 1.0, 1.5, 2.5)[attempt % 5])
        if best is None or len(rounds) < len(best):
            best = rounds
        if len(best) <= bound:
            break
    assert len(best) <= MAX_ROUNDS
    return best


@functools.cache
def routing_tables():
    classes = demand_classes()
    index = np.zeros((1000,), np.int32)
    rows = np.zeros((len(classes), 2, 128), np.int32)
    for number, combo in enumerate(classes):
        ids = [lo * (7 - lo) // 2 + hi for lo, hi in combo]
        index[ids[0] + 10 * ids[1] + 100 * ids[2]] = number
        where = {
            (chip, which, piece): (chip, which * PIECES + piece)
            for chip in range(4)
            for which in range(2)
            for piece in range(PIECES)
        }
        flat = np.zeros((256,), np.int32)
        rounds = solve_class(combo)
        for step, taken in enumerate(rounds):
            for (source, target), piece in taken.items():
                across = 0 if source ^ target == 1 else 1
                chip, slot = where[piece]
                assert chip == source
                flat[source * FIELDS + 2 * step + across] = slot
                where[piece] = (target, 2 * PIECES + 2 * step + across)
        for (source, which, piece), (chip, slot) in where.items():
            assert chip == combo[source][which]
            flat[chip * FIELDS + 2 * MAX_ROUNDS + (source * 2 + which) * PIECES + piece] = slot
        flat[4 * FIELDS] = max(len(rounds), BASE_ROUNDS) - BASE_ROUNDS
        rows[number] = flat.reshape(2, 128)
    return (index, rows)


def route_kernel(place_ref, matching_ref, index_ref, rows_ref, out_ref, row, dest, swap, sem):
    place = place_ref[0]
    chip = place // 2
    core = place % 2
    for position in range(8):
        dest[matching_ref[position]] = position // 2
    key = 0
    for at in range(4):
        first, second = dest[2 * at], dest[2 * at + 1]
        swap[at] = (first > second).astype(jnp.int32)
        if at < 3:
            lo, hi = jnp.minimum(first, second), jnp.maximum(first, second)
            key = key + 10**at * (lo * (7 - lo) // 2 + hi)
    copy = pltpu.make_async_copy(rows_ref.at[index_ref[key]], row, sem)
    copy.start()
    copy.wait()

    def field(flat):
        return row[flat // 128, flat % 128]

    def local_id(slot):
        owner = (slot // PIECES) ^ swap[chip]
        near = jnp.where(owner == core, 0, PIECES) + slot % PIECES
        return jnp.where(slot < 2 * PIECES, near, slot)

    for step in range(2 * MAX_ROUNDS):
        out_ref[step] = local_id(field(chip * FIELDS + step))
    layer = matching_ref[place]
    which = (layer % 2) ^ swap[layer // 2]
    base = chip * FIELDS + 2 * MAX_ROUNDS + (layer // 2 * 2 + which) * PIECES
    for piece in range(PIECES):
        out_ref[2 * MAX_ROUNDS + piece] = local_id(field(base + piece))
    out_ref[2 * MAX_ROUNDS + PIECES] = field(jnp.int32(4 * FIELDS))


def find_route(place, matching):
    index, rows = routing_tables()
    smem = pl.BlockSpec(memory_space=pltpu.SMEM)
    return pl.pallas_call(
        route_kernel,
        out_shape=jax.ShapeDtypeStruct((32,), jnp.int32),
        in_specs=[smem, smem, smem, pl.BlockSpec(memory_space=pl.ANY)],
        out_specs=smem,
        scratch_shapes=[
            pltpu.SMEM((2, 128), jnp.int32),
            pltpu.SMEM((8,), jnp.int32),
            pltpu.SMEM((4,), jnp.int32),
            pltpu.SemaphoreType.DMA,
        ],
    )(place, matching, jnp.asarray(index), jnp.asarray(rows))


def write_kernel(
    rows, first_of, place_ref, lengths_ref, cache_ref, fresh_ref, *refs
):
    out_ref, held, wide, sem_in, sem_out = refs[-5:]
    first = first_of(place_ref[0])

    def copy_in(row):
        return pltpu.make_async_copy(cache_ref.at[0, first + row], held.at[row], sem_in.at[row])

    def copy_out(row):
        return pltpu.make_async_copy(held.at[row], out_ref.at[row], sem_out.at[row])

    for row in range(rows):
        copy_in(row).start()
    wide[...] = fresh_ref[0].astype(jnp.float32)
    for row in range(rows):
        copy_in(row).wait()
        length = lengths_ref[first + row]
        start = pl.multiple_of(length // 16 * 16, 16)
        tile = held[row, pl.ds(start, 16), :].astype(jnp.float32)
        fresh = wide[pl.ds(first + row, 1), :]
        places = lax.broadcasted_iota(jnp.int32, tile.shape, 0) + start
        tile = jnp.where(places == length, fresh, tile)
        held[row, pl.ds(start, 16), :] = tile.astype(held.dtype)
        copy_out(row).start()
    for row in range(rows):
        copy_out(row).wait()


def write_tokens(place, lengths, kv_cache, fresh, rows, first_of, after=()):
    smem = pl.BlockSpec(memory_space=pltpu.SMEM)
    shape = (rows,) + kv_cache.shape[2:]
    return pl.pallas_call(
        functools.partial(write_kernel, rows, first_of),
        out_shape=jax.ShapeDtypeStruct(shape, kv_cache.dtype),
        in_specs=[
            smem,
            smem,
            pl.BlockSpec(memory_space=pl.ANY),
            pl.BlockSpec(memory_space=pltpu.VMEM),
        ]
        + [pl.BlockSpec(memory_space=pl.ANY)] * len(after),
        out_specs=pl.BlockSpec(memory_space=pl.ANY),
        scratch_shapes=[
            pltpu.VMEM(shape, kv_cache.dtype),
            pltpu.VMEM(fresh.shape[1:], jnp.float32),
            pltpu.SemaphoreType.DMA((rows,)),
            pltpu.SemaphoreType.DMA((rows,)),
        ],
        cost_estimate=pl.CostEstimate(
            flops=2 * math.prod(shape), bytes_accessed=4 * math.prod(shape), transcendentals=0
        ),
    )(place, lengths, kv_cache, fresh, *after)


def pick_kernel(step, n_near, n_after, ids_ref, *refs):
    outs, sems = refs[-3:-1], refs[-1]
    refs = refs[n_after:-3]
    near = refs[:n_near]
    passed = (len(refs) - n_near) // 2
    relays = (refs[n_near : n_near + passed], refs[n_near + passed :])
    per = outs[0].shape[0]
    for way in range(2):
        wanted = ids_ref[2 * step + way]
        for number, ref in enumerate(near):

            @pl.when((wanted >= number * PIECES) & (wanted < (number + 1) * PIECES))
            def _(number=number, ref=ref, wanted=wanted, way=way):
                start = (wanted - number * PIECES) * per
                pltpu.make_async_copy(ref.at[pl.ds(start, per)], outs[way], sems.at[way]).start()

        for past, ref in enumerate(relays[way]):

            @pl.when(wanted == 2 * PIECES + 2 * past + 1 - way)
            def _(ref=ref, way=way):
                pltpu.make_async_copy(ref, outs[way], sems.at[way]).start()

    for way in range(2):
        pltpu.make_async_copy(near[0].at[pl.ds(0, per)], outs[way], sems.at[way]).wait()


def pick_pieces(ids, step, near, from_x, from_y, after=()):
    shape = (near[0].shape[0] // PIECES,) + near[0].shape[1:]
    anywhere = pl.BlockSpec(memory_space=pl.ANY)
    operands = list(after) + list(near) + list(from_y) + list(from_x)
    one = pltpu.VMEM(shape, near[0].dtype)
    vmem = pl.BlockSpec(memory_space=pltpu.VMEM)
    return pl.pallas_call(
        functools.partial(pick_kernel, step, len(near), len(after)),
        out_shape=(one, one),
        in_specs=[pl.BlockSpec(memory_space=pltpu.SMEM)] + [anywhere] * len(operands),
        out_specs=(vmem, vmem),
        scratch_shapes=[pltpu.SemaphoreType.DMA((2,))],
        cost_estimate=pl.CostEstimate(
            flops=2 * math.prod(shape), bytes_accessed=8 * math.prod(shape), transcendentals=0
        ),
    )(ids, *operands)


def place_kernel(lo, hi, per, near_at, far_at, place_ref, ids_ref, *refs):
    out_ref, held, sem_in, sem_out = refs[-4:]
    core = place_ref[0] % 2
    blocks = [
        (side, stream, piece)
        for stream in range(STREAMS)
        for side in range(2)
        for piece in range(PIECES)
    ]

    def row_of(side, stream, piece):
        half = core if side == 0 else 1 - core
        return half * (STREAMS * PIECES * per) + (stream * PIECES + piece) * per

    def move(at, side, stream, piece):
        wanted = ids_ref[2 * MAX_ROUNDS + piece]
        mine = (wanted >= lo) & (wanted < hi)
        for number in range(2):
            if lo < 2 * PIECES:

                @pl.when((wanted >= number * PIECES) & (wanted < (number + 1) * PIECES))
                def _(ref=refs[near_at[side][number][stream]]):
                    start = (wanted - number * PIECES) * per
                    pltpu.make_async_copy(
                        ref.at[pl.ds(start, per)], held.at[at], sem_in.at[at]
                    ).start()

        for slot, position in far_at[side][stream].items():
            if lo <= slot < hi:

                @pl.when(wanted == slot)
                def _(ref=refs[position]):
                    pltpu.make_async_copy(ref, held.at[at], sem_in.at[at]).start()

        return mine

    def copy_out(at, block):
        row = row_of(*block)
        return pltpu.make_async_copy(held.at[at], out_ref.at[0, pl.ds(row, per)], sem_out.at[at])

    mine = [move(at, *block) for at, block in enumerate(blocks)]
    for at, block in enumerate(blocks):

        @pl.when(mine[at])
        def _(at=at, block=block):
            pltpu.make_async_copy(
                out_ref.at[0, pl.ds(0, per)], held.at[at], sem_in.at[at]
            ).wait()
            copy_out(at, block).start()

    for at, block in enumerate(blocks):

        @pl.when(mine[at])
        def _(at=at, block=block):
            copy_out(at, block).wait()


def place_pieces(place, ids, lo, hi, near, far, result, out_shape, after=()):
    operands = []
    near_at = [[[0, 0] for _ in range(2)] for _ in range(2)]
    far_at = [[{}, {}], [{}, {}]]

    def add(array):
        operands.append(array)
        return len(operands) - 1

    for side in range(2):
        for stream in range(STREAMS):
            if lo < 2 * PIECES:
                for owner in range(2):
                    near_at[side][owner][stream] = add(near[side][owner][stream])
            for slot, array in far[side][stream].items():
                if lo <= slot < hi:
                    far_at[side][stream][slot] = add(array)
    per = out_shape.shape[1] // (2 * STREAMS * PIECES)
    smem = pl.BlockSpec(memory_space=pltpu.SMEM)
    anywhere = pl.BlockSpec(memory_space=pl.ANY)
    operands += list(after)
    aliases = {}
    if result is not None:
        aliases = {2 + len(operands): 0}
        operands.append(result)
    count = 2 * STREAMS * PIECES
    return pl.pallas_call(
        functools.partial(place_kernel, lo, hi, per, near_at, far_at),
        out_shape=out_shape,
        in_specs=[smem, smem] + [anywhere] * len(operands),
        out_specs=anywhere,
        scratch_shapes=[
            pltpu.VMEM((count, per) + out_shape.shape[2:], out_shape.dtype),
            pltpu.SemaphoreType.DMA((count,)),
            pltpu.SemaphoreType.DMA((count,)),
        ],
        input_output_aliases=aliases,
        cost_estimate=pl.CostEstimate(
            flops=math.prod(out_shape.shape),
            bytes_accessed=2 * math.prod(out_shape.shape),
            transcendentals=0,
        ),
    )(place, ids, *operands)


def attend_kernel(block, lengths_ref, q_ref, cache_ref, fresh_ref, *refs):
    out_ref = refs[-1]
    base = pl.program_id(0) * block
    slots = cache_ref.shape[2]
    per_key = q_ref.shape[1]
    scores = []
    for row in range(block):
        length = lengths_ref[base + row]
        key = cache_ref[0, row, :, :HEAD_SIZE]
        query = q_ref[row]
        fresh_key = fresh_ref[0, row : row + 1, :HEAD_SIZE]
        s = lax.dot_general(
            query, key, (((1,), (1,)), ((), ())), preferred_element_type=jnp.float32
        )
        new = jnp.sum(
            query.astype(jnp.float32) * fresh_key.astype(jnp.float32), axis=1, keepdims=True
        )
        spots = lax.broadcasted_iota(jnp.int32, (per_key, slots), 1)
        s = jnp.where(spots == length, new, s) / math.sqrt(HEAD_SIZE)
        scores.append(jnp.where(spots <= length, s, -1e30))
    scores = jnp.stack(scores)
    scores = jnp.exp(scores - jnp.max(scores, axis=-1, keepdims=True))
    weights = scores / jnp.sum(scores, axis=-1, keepdims=True)
    for row in range(block):
        length = lengths_ref[base + row]
        weight = weights[row].astype(jnp.bfloat16)
        wide = weight.astype(jnp.float32)
        spots = lax.broadcasted_iota(jnp.int32, (per_key, slots), 1)
        at_new = jnp.sum(jnp.where(spots == length, wide, 0.0), axis=1, keepdims=True)
        rest = jnp.where(spots == length, 0.0, wide).astype(jnp.bfloat16)
        value = cache_ref[0, row, :, HEAD_SIZE:]
        fresh_value = fresh_ref[0, row : row + 1, HEAD_SIZE:].astype(jnp.float32)
        total = jnp.dot(rest, value, preferred_element_type=jnp.float32)
        out_ref[row] = (total + at_new * fresh_value).astype(out_ref.dtype)


def attend(head, lengths, queries, kv_cache, fresh, after=()):
    block = 8
    rows, slots = kv_cache.shape[1:3]
    kv_heads = kv_cache.shape[3] // (2 * HEAD_SIZE)
    per_key = queries.shape[1] // kv_heads
    work = rows * per_key * slots * HEAD_SIZE
    return pl.pallas_call(
        functools.partial(attend_kernel, block),
        out_shape=jax.ShapeDtypeStruct((rows, per_key, HEAD_SIZE), jnp.bfloat16),
        grid_spec=pltpu.PrefetchScalarGridSpec(
            num_scalar_prefetch=1,
            grid=(rows // block,),
            in_specs=[
                pl.BlockSpec((block, per_key, HEAD_SIZE), lambda i, _: (i, head, 0)),
                pl.BlockSpec((1, block, slots, 2 * HEAD_SIZE), lambda i, _: (0, i, 0, head)),
                pl.BlockSpec((1, block, 2 * HEAD_SIZE), lambda i, _: (0, i, head)),
            ]
            + [pl.BlockSpec(memory_space=pl.ANY)] * len(after),
            out_specs=pl.BlockSpec((block, per_key, HEAD_SIZE), lambda i, _: (i, 0, 0)),
        ),
        cost_estimate=pl.CostEstimate(
            flops=30 * work, bytes_accessed=rows * slots * 4 * HEAD_SIZE, transcendentals=0
        ),
    )(lengths, queries, kv_cache, fresh, *after)


def add_kernel(parts_ref, residual_ref, stream_ref, squares_ref):
    total = residual_ref[0].astype(jnp.float32)
    added = parts_ref[0].astype(jnp.float32)
    for part in range(1, parts_ref.shape[0]):
        added = added + parts_ref[part].astype(jnp.float32)
    total = total + added
    stream_ref[...] = total
    squares = jnp.sum(total * total, axis=-1, keepdims=True)
    squares_ref[...] = jnp.broadcast_to(squares, squares_ref.shape)


def add_parts_kernel(parts, residual):
    rows, width = residual.shape[1:]
    return pl.pallas_call(
        add_kernel,
        out_shape=(
            jax.ShapeDtypeStruct((rows, width), jnp.float32),
            jax.ShapeDtypeStruct((rows, 128), jnp.float32),
        ),
        cost_estimate=pl.CostEstimate(
            flops=8 * parts.size, bytes_accessed=2 * parts.size, transcendentals=0
        ),
    )(parts, residual)


def norm_kernel(groups, stream_ref, gain_ref, *refs):
    both_ref = refs[-1]
    stream = stream_ref[...]
    squares = refs[0][:, :1]
    for ref in refs[1:-1]:
        squares = squares + ref[:, :1]
    normed = stream * lax.rsqrt(squares / D + 1e-05) * gain_ref[...].astype(jnp.float32)
    per = stream.shape[0] // groups
    for group in range(groups):
        chunk = slice(group * per, (group + 1) * per)
        pair = jnp.concatenate([stream[chunk], normed[chunk]], axis=0)
        both_ref[group] = pair.astype(both_ref.dtype)


def norm_both(groups, stream, norm_gain, squares):
    rows, width = stream.shape
    return pl.pallas_call(
        functools.partial(norm_kernel, groups),
        out_shape=jax.ShapeDtypeStruct((groups, 2 * rows // groups, width), jnp.bfloat16),
        cost_estimate=pl.CostEstimate(
            flops=60 * stream.size, bytes_accessed=8 * stream.size, transcendentals=0
        ),
    )(stream, norm_gain, *squares)


def part_kernel(landed_ref, stream_ref, normed_ref):
    groups, double = landed_ref.shape[:2]
    per = double // 2
    landed = landed_ref[...].astype(jnp.float32)
    for way, ref in enumerate((stream_ref, normed_ref)):
        chunks = [landed[group, way * per : (way + 1) * per] for group in range(groups)]
        ref[0] = jnp.concatenate(chunks, axis=0).astype(ref.dtype)


def part_both(landed):
    groups, double, width = landed.shape
    one = jax.ShapeDtypeStruct((1, groups * double // 2, width), landed.dtype)
    return pl.pallas_call(part_kernel, out_shape=(one, one))(landed)


def shift_pairs(size, shift):
    return [(at, (at + shift) % size) for at in range(size)]


def flip_pairs(size, mask):
    return [(at, at ^ mask) for at in range(size)]


def sum_over_tensor(value):
    size = lax.axis_size(TENSOR)
    total = value
    for shift in range(1, size):
        total = total + lax.ppermute(value, TENSOR, shift_pairs(size, shift))
    return total


def scatter_sum(partial_value):
    size = lax.axis_size(TENSOR)
    parts = lax.all_to_all(partial_value, TENSOR, split_axis=1, concat_axis=0, tiled=True)
    return jnp.sum(parts.reshape((size,) + (partial_value.shape[0], -1)), axis=0)


def norm_rows(stream, norm_gain):
    squares = sum_over_tensor(jnp.sum(stream * stream, axis=-1, keepdims=True))
    normed = stream * lax.rsqrt(squares / D + 1e-05) * norm_gain[0].astype(jnp.float32)
    return jnp.concatenate([stream.astype(jnp.bfloat16), normed.astype(jnp.bfloat16)], axis=1)


def spread_rows(matching, value):
    groups = lax.axis_size(SECTION)
    folded = value.reshape((groups, value.shape[0] // groups) + value.shape[1:])
    spread = lax.all_to_all(folded, SECTION, split_axis=0, concat_axis=0, tiled=True)
    return jnp.take(spread, matching, axis=0, mode="clip")


def gather_rows(chosen, shape):
    landed = lax.all_to_all(chosen, SECTION, split_axis=0, concat_axis=0, tiled=True)
    return landed.reshape(shape)


def move_by_two_exchanges(matching, value):
    return gather_rows(spread_rows(matching, value), value.shape)


def on_any_section(
    matching, lengths, queries, kv_cache, incoming_key_value, residual, out_weight, norm_gain
):
    place = lax.axis_index(SECTION).astype(jnp.int32).reshape(1)
    rows = kv_cache.shape[1]
    updated = write_tokens(
        place, lengths, kv_cache, incoming_key_value, rows, lambda _: 0
    )
    cache_out = move_by_two_exchanges(matching, updated)
    kv_heads = kv_cache.shape[3] // (2 * HEAD_SIZE)
    split_queries = queries.reshape(rows, -1, HEAD_SIZE)
    partial_value = 0.0
    depth = out_weight.shape[1] // kv_heads
    for head in range(kv_heads):
        attended = attend(head, lengths, split_queries, kv_cache, incoming_key_value)
        partial_value += jnp.dot(
            attended.reshape(rows, -1),
            out_weight[0, head * depth : (head + 1) * depth],
            preferred_element_type=jnp.float32,
        )
    stream = residual[0].astype(jnp.float32) + scatter_sum(partial_value)
    both = norm_rows(stream, norm_gain)
    both = move_by_two_exchanges(matching, both)
    width = both.shape[1] // 2
    return (cache_out[None], both[None, :, :width], both[None, :, width:])


def on_four_chips(
    matching, lengths, queries, kv_cache, incoming_key_value, residual, out_weight, norm_gain
):
    place = lax.axis_index(SECTION).astype(jnp.int32).reshape(1)
    sections = lax.axis_size(SECTION)
    across_core, across_x, across_y = (flip_pairs(sections, mask) for mask in (1, 2, 4))
    rows = kv_cache.shape[1]
    kv_heads = kv_cache.shape[3] // (2 * HEAD_SIZE)
    fresh = incoming_key_value
    part = rows // (2 * STREAMS)

    def swap(array):
        return lax.ppermute(array, SECTION, across_core)

    lent, kept, got = [], [], []

    def share(stream, after=()):
        lent.append(
            write_tokens(
                place, lengths, kv_cache, fresh, part,
                lambda p: (1 - p % 2) * (rows // 2) + stream * part, after,
            )
        )
        got.append(swap(lent[-1]))
        kept.append(
            write_tokens(
                place, lengths, kv_cache, fresh, part,
                lambda p: p % 2 * (rows // 2) + stream * part, [lent[-1]],
            )
        )

    ids = find_route(place, matching)

    from_x = [[] for _ in range(STREAMS)]
    from_y = [[] for _ in range(STREAMS)]
    far = [[{} for _ in range(STREAMS)] for _ in range(2)]

    def send(step, stream, from_x, from_y, kept, got, ids, after=()):
        out_x, out_y = pick_pieces(
            ids, step, (kept[stream], got[stream]), from_x[stream], from_y[stream], after
        )
        landed_x = lax.ppermute(out_x, SECTION, across_x)
        landed_y = lax.ppermute(out_y, SECTION, across_y)
        return ((landed_x, landed_y), out_x)

    def receive(step, stream, landed, from_x, from_y, far):
        for way, array in enumerate(landed):
            (from_x, from_y)[way][stream].append(array)
            slot = 2 * PIECES + 2 * step + way
            far[0][stream][slot] = array
            far[1][stream][slot] = swap(array)

    split_queries = queries.reshape(rows, -1, HEAD_SIZE)
    depth = out_weight.shape[1] // kv_heads
    work = types.SimpleNamespace(sent=None)

    def attend_head(head):
        work.attended = attend(
            head, lengths, split_queries, kv_cache, incoming_key_value, [work.sent]
        )
        return [work.attended]

    def project_head(head):
        product = jnp.dot(
            work.attended.reshape(rows, -1),
            out_weight[0, head * depth : (head + 1) * depth],
            preferred_element_type=jnp.float32,
        )
        work.partial = product if head == 0 else work.partial + product
        if head == kv_heads - 1:
            work.partial = work.partial.astype(jnp.bfloat16)
        return [work.partial]

    def add_parts():
        parts = lax.all_to_all(
            work.partial, TENSOR, split_axis=1, concat_axis=0, tiled=True
        )
        parts = parts.reshape(lax.axis_size(TENSOR), rows, -1)
        work.stream, squares = add_parts_kernel(parts, residual)
        tensors = lax.axis_size(TENSOR)
        work.squares = [squares] + [
            lax.ppermute(squares, TENSOR, shift_pairs(tensors, shift))
            for shift in range(1, tensors)
        ]
        return [work.stream]

    def norm_stream():
        work.both = norm_both(sections, work.stream, norm_gain, work.squares)
        return [work.both]

    def move_both():
        spread = lax.all_to_all(work.both, SECTION, split_axis=0, concat_axis=0, tiled=True)
        chosen = jnp.take(spread, matching, axis=0, mode="clip")
        work.landed = lax.all_to_all(
            chosen, SECTION, split_axis=0, concat_axis=0, tiled=True
        )
        return [chosen]

    def split_both():
        work.outs = part_both(work.landed)
        return [work.sent]

    chores = []
    for head in range(kv_heads):
        chores += [functools.partial(attend_head, head), functools.partial(project_head, head)]
    out_shape = jax.ShapeDtypeStruct(kv_cache.shape, kv_cache.dtype)
    early = 2 * PIECES + 4

    def place_early():
        lent_back = [swap(array) for array in kept]
        near = [[kept, got], [lent, lent_back]]
        work.result = place_pieces(place, ids, 0, early, near, far, None, out_shape, [work.sent])
        return add_parts()

    chores += [None, place_early, norm_stream, move_both, split_both]
    after = []
    for step in range(BASE_ROUNDS):
        for stream in range(STREAMS):
            settled = [far[1][stream][s] for s in far[1][stream] if s < 2 * PIECES + 2 * step - 2]
            if step == 0:
                share(stream, [work.sent] if stream else [])
            landed, work.sent = send(
                step, stream, from_x, from_y, kept, got, ids, after + settled[-2:]
            )
            receive(step, stream, landed, from_x, from_y, far)
            chore = chores.pop(0) if step + stream > 0 and chores else None
            after = chore() if chore else []
    for chore in filter(None, chores):
        after = chore()
    stream_out, normed_out = work.outs
    ready = 2 * PIECES + 2 * (BASE_ROUNDS - 1)
    result = place_pieces(
        place, ids, early, ready, None, far, work.result, out_shape, after
    )

    def finish(extra, place, ids, kept, got, from_x, from_y, far, result):
        from_x, from_y = [list(a) for a in from_x], [list(a) for a in from_y]
        far = [[dict(a) for a in side] for side in far]
        lo = ready
        for step in range(BASE_ROUNDS, BASE_ROUNDS + extra):
            for stream in range(STREAMS):
                landed, _ = send(step, stream, from_x, from_y, kept, got, ids)
                receive(step, stream, landed, from_x, from_y, far)
        if extra:
            mid = 2 * PIECES + 2 * (BASE_ROUNDS + extra - 1)
            result = place_pieces(place, ids, lo, mid, None, far, result, out_shape)
            lo = mid
        top = 2 * PIECES + 2 * (BASE_ROUNDS + extra)
        return place_pieces(place, ids, lo, top, None, far, result, out_shape)

    late = [[{s: a for s, a in d.items() if s >= ready} for d in side] for side in far]
    cache_out = lax.switch(
        ids[2 * MAX_ROUNDS + PIECES],
        [functools.partial(finish, extra) for extra in range(MAX_ROUNDS - BASE_ROUNDS + 1)],
        place, ids, kept, got, from_x, from_y, late, result,
    )
    return (cache_out, stream_out, normed_out)


def solution(mesh):
    four_chips = mesh.shape[SECTION] == 8
    return jax.shard_map(
        on_four_chips if four_chips else on_any_section,
        mesh=mesh,
        in_specs=(
            P(),
            P(),
            P(SECTION, None, TENSOR),
            P(SECTION, None, None, TENSOR),
            P(SECTION, None, TENSOR),
            P(SECTION, None, TENSOR),
            P(SECTION, TENSOR, None),
            P(SECTION, TENSOR),
        ),
        out_specs=(
            P(SECTION, None, None, TENSOR),
            P(SECTION, None, TENSOR),
            P(SECTION, None, TENSOR),
        ),
        check_vma=False,
    )
```
